8 devices in a mesh: hp: 2 (over z, y), cp: 4 (over x, core).
Axes of the slice: x: 2, y: 2, z: 1, core: 2. Of those that a mesh axis runs over, the one named last changes fastest.
Arguments:
- q: bfloat16 [8, 2048, 32, 128], P(None, ('cp', 'hp'))
- k: bfloat16 [8, 2048, 8, 128], P(None, ('cp', 'hp'))
- v: bfloat16 [8, 2048, 8, 128], P(None, ('cp', 'hp'))
- o: bfloat16 [8, 2048, 32, 128], P(None, ('cp', 'hp'))
- do: bfloat16 [8, 2048, 32, 128], P(None, ('cp', 'hp'))
- lse: float32 [8, 32, 2048], P(None, None, ('cp', 'hp'))
Outputs:
- output 1: bfloat16 [8, 2048, 32, 128], P(None, ('cp', 'hp'))
- output 2: bfloat16 [8, 2048, 8, 128], P(None, ('cp', 'hp'))
- output 3: bfloat16 [8, 2048, 8, 128], P(None, ('cp', 'hp'))
All inputs are finite; a program needn't handle non-finite values.
Results may differ from the reference program's by a relative error of at most 0.001.
Values are sent between devices in bfloat16 or wider.
A program may use at most 1 GiB of HBM per device.

```python
import jax
import jax.numpy as jnp
from jax import lax

B = 8
CHUNK = 256
HKV = 8
GROUP = 4
HEAD = 128
CP = 4

HQ = HKV * GROUP
S = 2 * CP * CHUNK
QB = min(CHUNK, 256)


def _positions():
    c = jnp.arange(2 * CP)
    t = jnp.where(c % 2 == 0, c // 2, 2 * CP - 1 - c // 2)
    return (t[:, None] * CHUNK + jnp.arange(CHUNK)[None, :]).reshape(-1)


def _split_q(x):
    return x.reshape(B, S, HKV, GROUP, HEAD).transpose(0, 2, 3, 1, 4).reshape(B * HKV, GROUP, S, HEAD)


def _split_kv(x):
    return x.transpose(0, 2, 1, 3).reshape(B * HKV, S, HEAD)


def _merge_q(x):
    return x.reshape(B, HKV, GROUP, S, HEAD).transpose(0, 3, 1, 2, 4).reshape(B, S, HQ, HEAD)


def _forward(q, k, v):
    pos = _positions()
    scale = HEAD ** -0.5

    def one(args):
        qh, kh, vh = args
        kf = kh.astype(jnp.float32)
        vf = vh.astype(jnp.float32)

        def body(_, c):
            qc = lax.dynamic_slice_in_dim(qh, c * QB, QB, axis=1).astype(jnp.float32)
            pc = lax.dynamic_slice_in_dim(pos, c * QB, QB)
            s = jnp.einsum('gqd,kd->gqk', qc, kf) * scale
            s = jnp.where(pos[None, :] <= pc[:, None], s, -jnp.inf)
            m = jnp.max(s, axis=-1, keepdims=True)
            e = jnp.exp(s - m)
            l = jnp.sum(e, axis=-1, keepdims=True)
            oc = jnp.einsum('gqk,kd->gqd', e / l, vf)
            return None, (oc, (m + jnp.log(l))[..., 0])

        _, (oc, lc) = lax.scan(body, None, jnp.arange(S // QB))
        return oc.transpose(1, 0, 2, 3).reshape(GROUP, S, HEAD), lc.transpose(1, 0, 2).reshape(GROUP, S)

    o, lse = lax.map(one, (_split_q(q), _split_kv(k), _split_kv(v)))
    return _merge_q(o).astype(jnp.bfloat16), lse.reshape(B, HQ, S)


def setup_inputs(seed: int = 0) -> dict:
    kq, kk, kv, kd = jax.random.split(jax.random.PRNGKey(seed), 4)
    q = jax.random.normal(kq, (B, S, HQ, HEAD), jnp.float32).astype(jnp.bfloat16)
    k = jax.random.normal(kk, (B, S, HKV, HEAD), jnp.float32).astype(jnp.bfloat16)
    v = jax.random.normal(kv, (B, S, HKV, HEAD), jnp.float32).astype(jnp.bfloat16)
    do = (jax.random.normal(kd, (B, S, HQ, HEAD), jnp.float32) * (S ** 0.5 / 8)).astype(jnp.bfloat16)
    o, lse = _forward(q, k, v)
    return {'q': q, 'k': k, 'v': v, 'o': o, 'do': do, 'lse': lse}


def reference(q, k, v, o, do, lse):
    pos = _positions()
    scale = HEAD ** -0.5
    dlt = jnp.sum(do.astype(jnp.float32) * o.astype(jnp.float32), axis=-1)
    dlt = dlt.reshape(B, S, HKV, GROUP).transpose(0, 2, 3, 1).reshape(B * HKV, GROUP, S)

    def one(args):
        qh, kh, vh, doh, lh, eh = args
        kf = kh.astype(jnp.float32)
        vf = vh.astype(jnp.float32)

        def body(carry, c):
            dk, dv = carry
            qc = lax.dynamic_slice_in_dim(qh, c * QB, QB, axis=1).astype(jnp.float32)
            dc = lax.dynamic_slice_in_dim(doh, c * QB, QB, axis=1).astype(jnp.float32)
            lc = lax.dynamic_slice_in_dim(lh, c * QB, QB, axis=1)
            ec = lax.dynamic_slice_in_dim(eh, c * QB, QB, axis=1)
            pc = lax.dynamic_slice_in_dim(pos, c * QB, QB)
            s = jnp.einsum('gqd,kd->gqk', qc, kf) * scale
            p = jnp.where(pos[None, :] <= pc[:, None], jnp.exp(s - lc[..., None]), 0.0)
            dv = dv + jnp.einsum('gqk,gqd->kd', p.astype(jnp.bfloat16).astype(jnp.float32), dc)
            dp = jnp.einsum('gqd,kd->gqk', dc, vf)
            ds = (p * (dp - ec[..., None])).astype(jnp.bfloat16).astype(jnp.float32)
            dq = jnp.einsum('gqk,kd->gqd', ds, kf) * scale
            dk = dk + jnp.einsum('gqk,gqd->kd', ds, qc) * scale
            return (dk, dv), dq

        zero = jnp.zeros((S, HEAD), jnp.float32)
        (dk, dv), dq = lax.scan(body, (zero, zero), jnp.arange(S // QB))
        return dq.transpose(1, 0, 2, 3).reshape(GROUP, S, HEAD), dk, dv

    dq, dk, dv = lax.map(one, (_split_q(q), _split_kv(k), _split_kv(v), _split_q(do), lse.reshape(B * HKV, GROUP, S), dlt))
    dk = dk.reshape(B, HKV, S, HEAD).transpose(0, 2, 1, 3)
    dv = dv.reshape(B, HKV, S, HEAD).transpose(0, 2, 1, 3)
    return _merge_q(dq).astype(jnp.bfloat16), dk.astype(jnp.bfloat16), dv.astype(jnp.bfloat16)
```

```python
import functools

import jax
import jax.numpy as jnp
from jax import lax
from jax.experimental import pallas as pl
from jax.experimental.layout import Layout, with_layout_constraint
from jax.experimental.pallas import tpu as pltpu
from jax.sharding import PartitionSpec as P

AXES = ('cp', 'hp')
CHUNKS = (1, 2, 2, 2, 1)
ORDER = (
    ('in', 0, ()), ('in', 1, ()), ('stat', 0, ()), ('in', 2, ()), ('out', 0, ()), ('in', 3, (0,)), ('out', 1, ()),
    ('out', 2, (1,)), ('in', 4, ()), ('out', 3, (2,)), ('out', 4, (3,)),
)


def _dot(a, b, ca, cb):
    return lax.dot_general(a, b, (((ca,), (cb,)), ((), ())), preferred_element_type=jnp.float32)


def _kernel(n, g, scale, q_ref, do_ref, kv_ref, st_ref, out_ref, dk_ref, dv_ref, dq_ref):
    i = pl.program_id(1)
    t, d = q_ref.shape[-2:]

    def stored(j):
        return jnp.where(j < n // 2, 2 * j, 2 * n - 1 - 2 * j)

    @pl.when(i == 0)
    def _():
        dk_ref[...] = jnp.zeros_like(dk_ref)
        dv_ref[...] = jnp.zeros_like(dv_ref)

    dq_ref[...] = jnp.zeros_like(dq_ref)

    def step(j, diagonal):
        c = stored(j)
        q = q_ref[0, 0].reshape(g * t, d)
        do = do_ref[0, 0].reshape(g * t, d)
        k = kv_ref[c, 0, 0]
        v = kv_ref[c, 0, 1]
        p = jnp.exp(_dot(k, q, 1, 1) * scale - st_ref[0, 0, 0:1, :])
        if diagonal:
            key = lax.broadcasted_iota(jnp.int32, p.shape, 0)
            query = lax.broadcasted_iota(jnp.int32, p.shape, 1) & (t - 1)
            p = jnp.where(key <= query, p, 0.0)
        dv_ref[j] += _dot(p.astype(jnp.bfloat16), do, 1, 0)
        dp = _dot(v, do, 1, 1)
        ds = (p * (dp - st_ref[0, 0, 1:2, :])).astype(jnp.bfloat16)
        dk_ref[j] += _dot(ds, q, 1, 0)
        dq_ref[...] += _dot(ds, k, 0, 0)

    lax.fori_loop(0, i, lambda j, _: step(j, False), None)
    step(i, True)
    out_ref[stored(i), 0, 0:g] = (dq_ref[...] * scale).reshape(g, t, d).astype(out_ref.dtype)

    @pl.when(i == n - 1)
    def _():
        for j in range(n):
            c = 2 * j if j < n // 2 else 2 * n - 1 - 2 * j
            out_ref[c, 0, g] = (dk_ref[j] * scale).astype(out_ref.dtype)
            out_ref[c, 0, g + 1] = dv_ref[j].astype(out_ref.dtype)


def _attend(x, st, first, g, scale):
    n, nb, _, t, d = x.shape

    def stored(i):
        return jnp.where(i < n // 2, 2 * i, 2 * n - 1 - 2 * i)

    pairs = nb * n * (n + 1) // 2 * g * t * t
    return pl.pallas_call(
        functools.partial(_kernel, n, g, scale),
        grid=(nb, n),
        in_specs=[
            pl.BlockSpec((1, 1, g, t, d), lambda b, i: (stored(i), b, 0, 0, 0)),
            pl.BlockSpec((1, 1, g, t, d), lambda b, i: (stored(i), b, 1, 0, 0)),
            pl.BlockSpec((n, 1, 2, t, d), lambda b, i: (0, b, g, 0, 0)),
            pl.BlockSpec((1, 1, 2, g * t), lambda b, i: (stored(i), b + first, 0, 0)),
        ],
        out_specs=pl.BlockSpec((n, 1, g + 2, t, d), lambda b, i: (0, b, 0, 0, 0)),
        out_shape=jax.ShapeDtypeStruct((n, nb, g + 2, t, d), jnp.bfloat16),
        scratch_shapes=[
            pltpu.VMEM((n, t, d), jnp.float32),
            pltpu.VMEM((n, t, d), jnp.float32),
            pltpu.VMEM((g * t, d), jnp.float32),
        ],
        compiler_params=pltpu.CompilerParams(dimension_semantics=('arbitrary', 'arbitrary')),
        cost_estimate=pl.CostEstimate(flops=10 * pairs * d, bytes_accessed=x.size * 4, transcendentals=pairs),
        name='attend',
    )(x, x, x, st)


def solution(mesh):
    n = mesh.shape['cp'] * mesh.shape['hp']
    seq = P(None, AXES, None, None)
    stat = P(None, None, AXES)

    def body(q, k, v, o, do, lse):
        b, t, hq, d = q.shape
        hk = k.shape[2]
        g = hq // hk
        scale = d ** -0.5

        def heads(x, lo, hi):
            x = x[lo:hi]
            return x.reshape(hi - lo, t, hk, -1, d).transpose(2, 0, 3, 1, 4)

        def exchange(x):
            return lax.all_to_all(x, AXES, 0, 0, tiled=True)

        bounds = []
        lo = 0
        for size in CHUNKS:
            bounds.append((lo, lo + size))
            lo += size

        def pack(c):
            return jnp.concatenate([heads(x, *bounds[c]) for x in (q, do, k, v)], axis=2)

        def rows(x):
            return with_layout_constraint(x, Layout(major_to_minor=(0, 1, 2, 3)))

        def unpack(y, c, outs):
            lo, hi = bounds[c]
            new = [
                rows(y[:, :, :g].transpose(1, 3, 0, 2, 4).reshape(hi - lo, t, hq, d)),
                rows(y[:, :, g].transpose(1, 2, 0, 3)),
                rows(y[:, :, g + 1].transpose(1, 2, 0, 3)),
            ]
            if outs is None:
                zero = jnp.zeros((), q.dtype)
                return [lax.pad(x, zero, [(lo, b - hi, 0)] + [(0, 0, 0)] * 3) for x in new]
            return [lax.dynamic_update_slice(out, x, (lo, 0, 0, 0)) for out, x in zip(outs, new)]

        got, back, ahead, st, outs, last, prev = {}, {}, {}, None, None, None, None
        for kind, c, done in ORDER:
            if kind == 'in':
                x = ahead[c] if c in ahead else pack(c)
            elif kind == 'out':
                x = _attend(got[c], st, bounds[c][0], g, scale)
            else:
                dlt = jnp.sum(do.astype(jnp.float32) * o.astype(jnp.float32), axis=-1).transpose(0, 2, 1)
                x = jnp.stack([z.reshape(b, hk, g * t).transpose(1, 0, 2) for z in (lse, dlt)], axis=2)
                x, ahead[2] = lax.optimization_barrier((x, pack(2)))
            if last is not None:
                x, last, outs = lax.optimization_barrier((x, last, outs))
                if prev[0] == 'in':
                    got[prev[1]] = last
                elif prev[0] == 'out':
                    back[prev[1]] = last
                else:
                    st = last
            for e in done:
                back[e], x = lax.optimization_barrier((back[e], x))
                outs = unpack(back[e], e, outs)
            last = exchange(x)
            if kind == 'out':
                last = with_layout_constraint(last, Layout(major_to_minor=(0, 1, 2, 3, 4)))
            prev = kind, c
        dq, dk, dv = unpack(last, prev[1], outs)
        return dq, dk, dv

    return jax.shard_map(body, mesh=mesh, in_specs=(seq, seq, seq, seq, seq, stat), out_specs=(seq, seq, seq), check_vma=False)
```

```python
import functools

import jax
import jax.numpy as jnp
from jax import lax
from jax.experimental import pallas as pl
from jax.experimental.layout import Layout, with_layout_constraint
from jax.experimental.pallas import tpu as pltpu
from jax.sharding import PartitionSpec as P

AXES = ('cp', 'hp')
CHUNKS = (1, 3, 3, 1)
ORDER = (
    ('in', 0, ()), ('in', 1, ()), ('stat', 0, ()), ('in', 2, ()), ('out', 0, ()), ('in', 3, (0,)), ('out', 1, ()),
    ('out', 2, (1,)), ('out', 3, (2,)),
)


def _dot(a, b, ca, cb):
    return lax.dot_general(a, b, (((ca,), (cb,)), ((), ())), preferred_element_type=jnp.float32)


def _kernel(n, g, scale, q_ref, do_ref, kv_ref, st_ref, out_ref, dk_ref, dv_ref, dq_ref):
    i = pl.program_id(1)
    t, d = q_ref.shape[-2:]

    def stored(j):
        return jnp.where(j < n // 2, 2 * j, 2 * n - 1 - 2 * j)

    @pl.when(i == 0)
    def _():
        dk_ref[...] = jnp.zeros_like(dk_ref)
        dv_ref[...] = jnp.zeros_like(dv_ref)

    dq_ref[...] = jnp.zeros_like(dq_ref)

    def step(j, diagonal):
        c = stored(j)
        q = q_ref[0, 0].reshape(g * t, d)
        do = do_ref[0, 0].reshape(g * t, d)
        k = kv_ref[c, 0, 0]
        v = kv_ref[c, 0, 1]
        p = jnp.exp(_dot(k, q, 1, 1) * scale - st_ref[0, 0, 0:1, :])
        if diagonal:
            key = lax.broadcasted_iota(jnp.int32, p.shape, 0)
            query = lax.broadcasted_iota(jnp.int32, p.shape, 1) & (t - 1)
            p = jnp.where(key <= query, p, 0.0)
        dv_ref[j] += _dot(p.astype(jnp.bfloat16), do, 1, 0)
        dp = _dot(v, do, 1, 1)
        ds = (p * (dp - st_ref[0, 0, 1:2, :])).astype(jnp.bfloat16)
        dk_ref[j] += _dot(ds, q, 1, 0)
        dq_ref[...] += _dot(ds, k, 0, 0)

    lax.fori_loop(0, i, lambda j, _: step(j, False), None)
    step(i, True)
    out_ref[stored(i), 0, 0:g] = (dq_ref[...] * scale).reshape(g, t, d).astype(out_ref.dtype)

    @pl.when(i == n - 1)
    def _():
        for j in range(n):
            c = 2 * j if j < n // 2 else 2 * n - 1 - 2 * j
            out_ref[c, 0, g] = (dk_ref[j] * scale).astype(out_ref.dtype)
            out_ref[c, 0, g + 1] = dv_ref[j].astype(out_ref.dtype)


def _attend(x, st, first, g, scale):
    n, nb, _, t, d = x.shape

    def stored(i):
        return jnp.where(i < n // 2, 2 * i, 2 * n - 1 - 2 * i)

    pairs = nb * n * (n + 1) // 2 * g * t * t
    return pl.pallas_call(
        functools.partial(_kernel, n, g, scale),
        grid=(nb, n),
        in_specs=[
            pl.BlockSpec((1, 1, g, t, d), lambda b, i: (stored(i), b, 0, 0, 0)),
            pl.BlockSpec((1, 1, g, t, d), lambda b, i: (stored(i), b, 1, 0, 0)),
            pl.BlockSpec((n, 1, 2, t, d), lambda b, i: (0, b, g, 0, 0)),
            pl.BlockSpec((1, 1, 2, g * t), lambda b, i: (stored(i), b + first, 0, 0)),
        ],
        out_specs=pl.BlockSpec((n, 1, g + 2, t, d), lambda b, i: (0, b, 0, 0, 0)),
        out_shape=jax.ShapeDtypeStruct((n, nb, g + 2, t, d), jnp.bfloat16),
        scratch_shapes=[
            pltpu.VMEM((n, t, d), jnp.float32),
            pltpu.VMEM((n, t, d), jnp.float32),
            pltpu.VMEM((g * t, d), jnp.float32),
        ],
        compiler_params=pltpu.CompilerParams(dimension_semantics=('arbitrary', 'arbitrary')),
        cost_estimate=pl.CostEstimate(flops=10 * pairs * d, bytes_accessed=x.size * 4, transcendentals=pairs),
        name='attend',
    )(x, x, x, st)


def solution(mesh):
    n = mesh.shape['cp'] * mesh.shape['hp']
    seq = P(None, AXES, None, None)
    stat = P(None, None, AXES)

    def body(q, k, v, o, do, lse):
        b, t, hq, d = q.shape
        hk = k.shape[2]
        g = hq // hk
        scale = d ** -0.5

        def heads(x, lo, hi):
            x = x[lo:hi]
            return x.reshape(hi - lo, t, hk, -1, d).transpose(2, 0, 3, 1, 4)

        def exchange(x):
            return lax.all_to_all(x, AXES, 0, 0, tiled=True)

        bounds = []
        lo = 0
        for size in CHUNKS:
            bounds.append((lo, lo + size))
            lo += size

        def pack(c):
            return jnp.concatenate([heads(x, *bounds[c]) for x in (q, do, k, v)], axis=2)

        def rows(x):
            return with_layout_constraint(x, Layout(major_to_minor=(0, 1, 2, 3)))

        def unpack(y, c, outs):
            lo, hi = bounds[c]
            new = [
                rows(y[:, :, :g].transpose(1, 3, 0, 2, 4).reshape(hi - lo, t, hq, d)),
                rows(y[:, :, g].transpose(1, 2, 0, 3)),
                rows(y[:, :, g + 1].transpose(1, 2, 0, 3)),
            ]
            if outs is None:
                zero = jnp.zeros((), q.dtype)
                return [lax.pad(x, zero, [(lo, b - hi, 0)] + [(0, 0, 0)] * 3) for x in new]
            return [lax.dynamic_update_slice(out, x, (lo, 0, 0, 0)) for out, x in zip(outs, new)]

        def attend(c):
            return _attend(got[c], st, bounds[c][0], g, scale)

        got, back, ahead, ahead_out, st, outs, last, prev = {}, {}, {}, {}, None, None, None, None
        for kind, c, done in ORDER:
            if kind == 'in':
                x = ahead[c] if c in ahead else pack(c)
            elif kind == 'out':
                x = ahead_out[c] if c in ahead_out else attend(c)
                if c == 0:
                    x, ahead_out[1] = lax.optimization_barrier((x, attend(1)))
            else:
                dlt = jnp.sum(do.astype(jnp.float32) * o.astype(jnp.float32), axis=-1).transpose(0, 2, 1)
                x = jnp.stack([z.reshape(b, hk, g * t).transpose(1, 0, 2) for z in (lse, dlt)], axis=2)
                x, ahead[2] = lax.optimization_barrier((x, pack(2)))
            if last is not None:
                x, last, outs = lax.optimization_barrier((x, last, outs))
                if prev[0] == 'in':
                    got[prev[1]] = last
                elif prev[0] == 'out':
                    back[prev[1]] = last
                else:
                    st = last
            for e in done:
                back[e], x = lax.optimization_barrier((back[e], x))
                outs = unpack(back[e], e, outs)
            last = exchange(x)
            if kind == 'out':
                last = with_layout_constraint(last, Layout(major_to_minor=(0, 1, 2, 3, 4)))
            prev = kind, c
        dq, dk, dv = unpack(last, prev[1], outs)
        return dq, dk, dv

    return jax.shard_map(body, mesh=mesh, in_specs=(seq, seq, seq, seq, seq, stat), out_specs=(seq, seq, seq), check_vma=False)
```
